32 devices in a mesh: groups: 2 (over x), steps: 8 (over z, y), inner: 2 (over core).
Axes of the slice: x: 2, y: 2, z: 4, core: 2. Of those that a mesh axis runs over, the one named last changes fastest.
Arguments:
- start_state: float32 [16, 32, 768], P('groups'), parts along dimension 0, may hold values from -6 to 6
- noise_draws: float32 [32, 8, 32, 768], P(('groups', 'steps', 'inner')), parts along dimension 0, may hold values from -6 to 6
- step_gaps: int32 [32], P(('groups', 'steps', 'inner')), parts along dimension 0, may hold values from 1 to 15
- window_start: int32 [2], P('groups'), parts along dimension 0, may hold values from 240 to 999
- input_weight: bfloat16 [768, 1024], replicated, may hold values from -0.21875 to 0.21875
- embed_weight: bfloat16 [256, 2048], replicated, may hold values from -0.375 to 0.375
- first_weight: bfloat16 [1024, 1024], replicated, may hold values from -0.1875 to 0.1875
- second_weight: bfloat16 [1024, 1024], replicated, may hold values from -0.1875 to 0.1875
- output_weight: bfloat16 [1024, 768], replicated, may hold values from -0.1875 to 0.1875
Outputs:
- trajectory: float32 [32, 8, 32, 768], P(('groups', 'steps', 'inner')), parts along dimension 0
The draws below stay inside these ranges and needn't reach their ends.
There are 2 independent parts, one for each index of `groups`. The reference program is written for one: setup_inputs(seed, part) draws one part's arguments, and reference() takes and returns one part's arrays. A program takes and returns all parts, laid end to end along the dimension named above; an argument that names none is the same for every part. Nothing has to cross between parts.
All inputs are finite; a program needn't handle non-finite values.
Results may differ from the reference program's by a relative error of at most 0.00035.
Values sent between devices are 32-bit elements; how exact they have to be, the bound alone decides.
A program may use at most 64 MiB of HBM per device.

```python
import math
import jax
import jax.numpy as jnp
from jax import lax

BATCH = 8
PATCHES = 32
FEATURES = 768
CHANNELS = 1024
FREQS = 128
GROUPS = 32
ITERS = 2
GAP_MAX = 15
TRAIN_STEPS = 1000
WINDOW = 16


def place_ends(array, rng, low, high):
    place = [jax.random.randint(jax.random.fold_in(rng, axis), (), 0, length) for axis, length in enumerate(array.shape)]
    main_axis = array.shape.index(max(array.shape))
    neighbour = place[:main_axis] + [(place[main_axis] + 1) % array.shape[main_axis]] + place[main_axis + 1:]
    return array.at[tuple(place)].set(low).at[tuple(neighbour)].set(high)


def shard_levels(stream_key, dims, split, least, largest):
    def one(position, shards_of):
        heights = jax.random.uniform(jax.random.fold_in(jax.random.fold_in(stream_key, 6), position), (shards_of,), jnp.float32, least / len(split), largest / len(split))
        return jnp.repeat(jnp.exp(heights), dims[position] // shards_of).reshape((-1,) + (1,) * (len(dims) - position - 1))

    level = one(*split[0])
    for cut in split[1:]:
        level = level * one(*cut)
    return level


def scatter_about(own_key, shape, deviation, bound, cuts=(), held_as=jnp.bfloat16):
    drawn = deviation * jax.random.normal(own_key, shape, jnp.float32)
    if cuts:
        drawn = drawn * shard_levels(own_key, shape, cuts, -0.22, 0.18)
    return jnp.clip(drawn, -bound, bound).astype(held_as)


def setup_inputs(seed: int = 0, part: int = 0) -> dict:
    key_list = jax.random.split(jax.random.key(seed), 10)
    part_keys = jax.random.split(jax.random.fold_in(key_list[9], part), 10)
    start_state = scatter_about(part_keys[0], (BATCH, PATCHES, FEATURES), 1.0, 6.0, (), jnp.float32)
    noise_draws = scatter_about(part_keys[1], (WINDOW, BATCH, PATCHES, FEATURES), 1.0, 6.0, ((0, 16),), jnp.float32)
    step_gaps = place_ends(jax.random.randint(part_keys[2], (WINDOW,), 1, GAP_MAX + 1), jax.random.fold_in(part_keys[2], 1), 1, GAP_MAX).astype(jnp.int32)
    window_start = jax.random.randint(part_keys[3], (1,), WINDOW * GAP_MAX, TRAIN_STEPS).astype(jnp.int32)
    input_weight = scatter_about(key_list[4], (FEATURES, CHANNELS), FEATURES ** -0.5, 0.21875)
    embed_weight = scatter_about(key_list[5], (2 * FREQS, 2 * CHANNELS), (2 * FREQS) ** -0.5, 0.375)
    first_weight = scatter_about(key_list[6], (CHANNELS, CHANNELS), CHANNELS ** -0.5, 0.1875)
    second_weight = scatter_about(key_list[7], (CHANNELS, CHANNELS), CHANNELS ** -0.5, 0.1875)
    output_weight = scatter_about(key_list[8], (CHANNELS, FEATURES), CHANNELS ** -0.5, 0.1875)
    return dict(start_state=start_state, noise_draws=noise_draws, step_gaps=step_gaps, window_start=window_start, input_weight=input_weight, embed_weight=embed_weight, first_weight=first_weight, second_weight=second_weight, output_weight=output_weight)


def noise_table():
    levels = jnp.arange(TRAIN_STEPS, dtype=jnp.float32)
    beta_values = 0.0001 + (0.02 - 0.0001) * levels / (TRAIN_STEPS - 1)
    return jnp.exp(jnp.cumsum(jnp.log1p(-beta_values)))

def lookup(table, noise_level):
    places = jnp.arange(TRAIN_STEPS, dtype=jnp.int32)
    return jnp.sum(jnp.where(places == noise_level, table, jnp.zeros_like(table)))

def group_norm(hidden, batch_count):
    total_rows, channel_count = hidden.shape
    shaped = hidden.reshape(batch_count, total_rows // batch_count, channel_count)

    def group_mean(values):
        per_channel = lax.optimization_barrier(jnp.mean(values, axis=1)).reshape(batch_count, GROUPS, channel_count // GROUPS)
        per_group = lax.optimization_barrier(jnp.mean(per_channel, axis=2, keepdims=True))
        return jnp.broadcast_to(per_group, per_channel.shape).reshape(batch_count, 1, channel_count)
    center = group_mean(shaped)
    offset = shaped - center
    spread = group_mean(offset * offset)
    return (offset * lax.rsqrt(spread + 1e-05)).reshape(total_rows, channel_count)

def predict_noise(state, noise_level, input_weight, embed_weight, first_weight, second_weight, output_weight):
    batch_count, patch_count, feature_count = state.shape
    channel_count = input_weight.shape[1]
    flat_state = state.reshape(batch_count * patch_count, feature_count).astype(jnp.bfloat16)
    entry_hidden = jnp.dot(flat_state, input_weight, preferred_element_type=jnp.float32)
    half_count = embed_weight.shape[0] // 2
    frequency = jnp.exp(-math.log(10000.0) * jnp.arange(half_count, dtype=jnp.float32) / half_count)
    angles = noise_level.astype(jnp.float32) * frequency
    features = jnp.concatenate([jnp.cos(angles), jnp.sin(angles)])[None, :].astype(jnp.bfloat16)
    modulation = jnp.dot(features, embed_weight, preferred_element_type=jnp.float32)
    scale_part = modulation[:, :channel_count]
    shift_part = modulation[:, channel_count:]
    act_one = jax.nn.silu(group_norm(entry_hidden, batch_count) * (1.0 + scale_part) + shift_part).astype(jnp.bfloat16)
    middle = jnp.dot(act_one, first_weight, preferred_element_type=jnp.float32)
    act_two = jax.nn.silu(group_norm(middle, batch_count)).astype(jnp.bfloat16)
    block_out = entry_hidden + jnp.dot(act_two, second_weight, preferred_element_type=jnp.float32)
    act_three = jax.nn.silu(group_norm(block_out, batch_count)).astype(jnp.bfloat16)
    predicted = jnp.dot(act_three, output_weight, preferred_element_type=jnp.float32)
    return predicted.reshape(state.shape)

def drift_of(state, noise_draw, level_now, level_next, table, input_weight, embed_weight, first_weight, second_weight, output_weight):
    predicted = predict_noise(state, level_now, input_weight, embed_weight, first_weight, second_weight, output_weight)
    bar_now = lookup(table, level_now)
    bar_next = lookup(table, level_next)
    clean_guess = jnp.clip((state - jnp.sqrt(1.0 - bar_now) * predicted) / jnp.sqrt(bar_now), -1.0, 1.0)
    implied = (state - jnp.sqrt(bar_now) * clean_guess) / jnp.sqrt(1.0 - bar_now)
    sigma_value = jnp.sqrt((1.0 - bar_next) / (1.0 - bar_now) * (1.0 - bar_now / bar_next))
    noise_coef = (1.0 - bar_next) * jnp.sqrt(bar_now / (bar_next * (1.0 - bar_now)))
    return jnp.sqrt(bar_next) * clean_guess + noise_coef * implied + sigma_value * noise_draw - state

def reference(start_state, noise_draws, step_gaps, window_start, input_weight, embed_weight, first_weight, second_weight, output_weight):
    table = noise_table()
    before = jnp.cumsum(step_gaps) - step_gaps
    level_now = (window_start[0] - before).astype(jnp.int32)
    level_next = (level_now - step_gaps).astype(jnp.int32)
    states = jnp.broadcast_to(start_state[None], noise_draws.shape)

    def one_step(item):
        return drift_of(item[0], item[1], item[2], item[3], table, input_weight, embed_weight, first_weight, second_weight, output_weight)
    totals = states
    for iteration in range(ITERS):
        drifts = lax.map(one_step, (states, noise_draws, level_now, level_next))
        totals = jnp.cumsum(drifts, axis=0)
        states = start_state[None] + (totals - drifts)
    return start_state[None] + totals
```

```python
import functools
import math

import jax
import jax.numpy as jnp
import numpy as np
from jax import lax
from jax.experimental import pallas as pl
from jax.experimental.pallas import tpu as pltpu
from jax.sharding import PartitionSpec as P

GROUPS = 32
ITERS = 2
TRAIN_STEPS = 1000
CHUNK_IMAGES = 2
LANES = 128
BLOCK = 256
MESH = pl.DeviceIdType.MESH
F32 = jnp.float32
BF16 = jnp.bfloat16


def noise_table():
    levels = np.arange(TRAIN_STEPS, dtype=np.float32)
    beta = (0.0001 + (0.02 - 0.0001) * levels / (TRAIN_STEPS - 1)).astype(np.float32)
    bars = np.exp(np.cumsum(np.log1p(-beta.astype(np.float64)))).astype(np.float32)
    padded = np.zeros((-(-TRAIN_STEPS // (8 * LANES)) * 8 * LANES,), np.float32)
    padded[:TRAIN_STEPS] = bars
    return padded.reshape(-1, LANES)


def frequencies(count):
    powers = -math.log(10000.0) * np.arange(count, dtype=np.float32) / count
    return np.exp(powers.astype(np.float32)).astype(np.float32)[None, :]


def group_matrix(channels, rows):
    width = channels // GROUPS
    place = np.arange(BLOCK) // width
    same = (place[:, None] == place[None, :]).astype(np.float32)
    return same / (width * rows)


def silu(value):
    half = 0.5 * value
    return half + half * jnp.tanh(half)


def kernel(
    cfg,
    gap_ref,
    start_level_ref,
    table_ref,
    freq_ref,
    group_ref,
    start_hbm,
    noise_hbm,
    win_hbm,
    wemb_hbm,
    w1_hbm,
    w2_hbm,
    wout_hbm,
    out_hbm,
    start_v,
    noise_v,
    win,
    wemb,
    w1,
    w2,
    wout,
    gap_send,
    gap_all,
    modulation_v,
    coef_v,
    drift_v,
    core_rx,
    chain_rx,
    chain_tx,
    side_rx,
    final_tx,
    prefix_v,
    out_v,
    load_sem,
    gap_send_sem,
    gap_recv_sem,
    core_send,
    core_recv,
    chain_send,
    chain_recv,
    side_send,
    side_recv,
    final_send,
    final_recv,
    out_sem,
):
    steps, inner, columns, chunks, size, patches, features, channels = cfg
    rows = steps // columns
    half = size // 2
    total = size * patches
    s = lax.axis_index("steps")
    h = lax.axis_index("inner")
    z, y = s // columns, lax.rem(s, columns)
    window = steps * inner
    me = s * inner + h
    messages = ITERS * chunks

    loads = [
        pltpu.make_async_copy(src, dst, load_sem.at[i])
        for i, (src, dst) in enumerate(
            [
                (start_hbm, start_v),
                (win_hbm, win),
                (wemb_hbm, wemb),
                (w1_hbm, w1),
                (w2_hbm, w2),
                (wout_hbm, wout),
                (noise_hbm, noise_v),
            ]
        )
    ]
    for load in loads:
        load.start()
    gap_send[...] = jnp.zeros_like(gap_send) + gap_ref[0]

    barrier = pltpu.get_barrier_semaphore()
    for j in range(1, window):
        to = lax.rem(me + j, window)
        pl.semaphore_signal(
            barrier,
            inc=1,
            device_id={"steps": to // inner, "inner": lax.rem(to, inner)},
            device_id_type=MESH,
        )
    pl.semaphore_wait(barrier, window - 1)

    def gap_copy(j):
        to = lax.rem(me + j, window)
        return pltpu.make_async_remote_copy(
            src_ref=gap_send,
            dst_ref=gap_all.at[me],
            send_sem=gap_send_sem.at[j],
            recv_sem=gap_recv_sem.at[me],
            device_id={"steps": to // inner, "inner": lax.rem(to, inner)},
            device_id_type=MESH,
        )

    def gap_arrival(j):
        origin = lax.rem(me + j, window)
        return pltpu.make_async_remote_copy(
            src_ref=gap_send,
            dst_ref=gap_all.at[origin],
            send_sem=gap_send_sem.at[j],
            recv_sem=gap_recv_sem.at[origin],
            device_id={"steps": origin // inner, "inner": lax.rem(origin, inner)},
            device_id_type=MESH,
        )

    for j in range(1, window):
        gap_copy(j).start()

    for n in range(chunks):
        prefix_v[n] = jnp.zeros(prefix_v.shape[1:], F32)

    @pl.when(z == 0)
    def _():
        chain_rx[...] = jnp.zeros_like(chain_rx)

    def core_copy(m):
        return pltpu.make_async_remote_copy(
            src_ref=drift_v.at[m, 1 - h],
            dst_ref=core_rx.at[m],
            send_sem=core_send.at[m],
            recv_sem=core_recv.at[m],
            device_id={"inner": 1 - h},
            device_id_type=MESH,
        )

    def chain_copy(m):
        return pltpu.make_async_remote_copy(
            src_ref=chain_tx.at[m],
            dst_ref=chain_rx.at[m],
            send_sem=chain_send.at[m],
            recv_sem=chain_recv.at[m],
            device_id={"steps": lax.rem(s + columns, steps)},
            device_id_type=MESH,
        )

    def side_copy(m, source):
        return pltpu.make_async_remote_copy(
            src_ref=source.at[m],
            dst_ref=side_rx.at[m],
            send_sem=side_send.at[m],
            recv_sem=side_recv.at[m],
            device_id={"steps": z * columns + (1 - y)},
            device_id_type=MESH,
        )

    def final_copy(m):
        return pltpu.make_async_remote_copy(
            src_ref=final_tx.at[m],
            dst_ref=prefix_v.at[m + chunks, h],
            send_sem=final_send.at[m],
            recv_sem=final_recv.at[m],
            device_id={"inner": 1 - h},
            device_id_type=MESH,
        )

    def final_arrival(m):
        return pltpu.make_async_remote_copy(
            src_ref=final_tx.at[m],
            dst_ref=prefix_v.at[m + chunks, 1 - h],
            send_sem=final_send.at[m],
            recv_sem=final_recv.at[m],
            device_id={"inner": 1 - h},
            device_id_type=MESH,
        )

    def out_copy(c):
        return pltpu.make_async_copy(out_v.at[c], out_hbm.at[c], out_sem.at[c])

    def chain(m):
        core_copy(m).wait_recv()

        @pl.when(z > 0)
        def _():
            chain_copy(m).wait_recv()

        chain_tx[m] = chain_rx[m] + (drift_v[m, h] + core_rx[m])

        @pl.when(z < rows - 1)
        def _():
            chain_copy(m).start()

        if columns == 2:

            @pl.when(y == 0)
            def _():
                side_copy(m, chain_tx).start()

            @pl.when(y == 1)
            def _():
                side_copy(m, chain_rx).start()

    def hand_back(m):
        prefix = chain_rx[m]
        if columns == 2:
            side_copy(m, chain_tx).wait_recv()
            prefix = prefix + side_rx[m]

        @pl.when(h == 0)
        def _():
            final_tx[m] = prefix + drift_v[m, 0]
            prefix_v[m + chunks, 0] = prefix

        @pl.when(h == 1)
        def _():
            final_tx[m] = prefix
            prefix_v[m + chunks, 1] = prefix + core_rx[m]

        final_copy(m).start()

    def finish(m):
        final_arrival(m).wait_recv()

    def group_average(partial):
        blocks = channels // BLOCK
        stacked = jnp.concatenate(
            [partial[:, i * BLOCK : (i + 1) * BLOCK] for i in range(blocks)], axis=0
        )
        matrix = group_ref[...]
        high = stacked.astype(BF16)
        rest = stacked - high.astype(F32)
        middle = rest.astype(BF16)
        low = (rest - middle.astype(F32)).astype(BF16)
        summed = (
            jnp.dot(low, matrix, preferred_element_type=F32)
            + jnp.dot(middle, matrix, preferred_element_type=F32)
            + jnp.dot(high, matrix, preferred_element_type=F32)
        )
        summed = jnp.sum(summed.reshape(blocks, size, 8, BLOCK), axis=2, keepdims=True)
        return jnp.concatenate([summed[i] for i in range(blocks)], axis=-1)

    def row_sums(value):
        return jnp.sum(value.reshape(size, patches // 8, 8, channels), axis=1).reshape(
            size * 8, channels
        )

    def centered(hidden):
        shaped = hidden.reshape(size, patches, channels)
        offset = shaped - group_average(row_sums(shaped))
        return offset, lax.rsqrt(group_average(row_sums(offset * offset)) + 1e-05)

    def set_level():
        for j in range(1, window):
            gap_arrival(j).wait_recv()
        earlier = jnp.zeros(gap_send.shape, jnp.int32)
        for k in range(window):
            earlier = earlier + jnp.where(k < me, gap_all[k], 0)
        level_now = start_level_ref[0] - earlier
        level_next = level_now - gap_ref[0]
        table = table_ref[...]
        places = lax.broadcasted_iota(jnp.int32, table.shape, 0) * LANES + (
            lax.broadcasted_iota(jnp.int32, table.shape, 1)
        )

        def lookup(level):
            found = jnp.where(places == level[:1, :1], table, 0.0)
            return jnp.sum(jnp.sum(found, axis=0, keepdims=True), axis=1, keepdims=True)

        bar_now, bar_next = lookup(level_now), lookup(level_next)
        coefs = [
            jnp.sqrt(1.0 - bar_now),
            1.0 / jnp.sqrt(bar_now),
            jnp.sqrt(bar_now),
            1.0 / jnp.sqrt(1.0 - bar_now),
            jnp.sqrt(bar_next),
            (1.0 - bar_next) * jnp.sqrt(bar_now / (bar_next * (1.0 - bar_now))),
            jnp.sqrt((1.0 - bar_next) / (1.0 - bar_now) * (1.0 - bar_now / bar_next)),
        ]
        for i, coef in enumerate(coefs):
            coef_v[i] = jnp.broadcast_to(coef, coef_v.shape[1:])
        angles = level_now.astype(F32)[:, :1] * freq_ref[...]
        around = jnp.concatenate([jnp.cos(angles), jnp.sin(angles)], axis=1).astype(BF16)
        loads[2].wait()
        modulation_v[...] = jnp.dot(around, wemb[...], preferred_element_type=F32)

    def compute(n):
        c = lax.rem(n, chunks)

        @pl.when(n == 0)
        def _():
            loads[0].wait()
            loads[1].wait()

        state = start_v[c] + prefix_v[n].reshape(size, patches, features)
        flat = state.reshape(total, features).astype(BF16)
        entry = jnp.dot(flat, win[...], preferred_element_type=F32)
        offset, spread = centered(entry)

        @pl.when(n == 0)
        def _():
            set_level()
            loads[3].wait()

        scale = modulation_v[:1, :channels].reshape(1, 1, channels)
        shift = modulation_v[:1, channels:].reshape(1, 1, channels)
        one = silu(offset * (spread * (1.0 + scale)) + shift).astype(BF16)
        middle = jnp.dot(one.reshape(total, channels), w1[...], preferred_element_type=F32)
        offset, spread = centered(middle)
        two = silu(offset * spread).astype(BF16)

        @pl.when(n == 0)
        def _():
            loads[4].wait()

        block = entry + jnp.dot(
            two.reshape(total, channels), w2[...], preferred_element_type=F32
        )
        offset, spread = centered(block)
        three = silu(offset * spread).astype(BF16)

        @pl.when(n == 0)
        def _():
            loads[5].wait()
            loads[6].wait()

        eps = jnp.dot(three.reshape(total, channels), wout[...], preferred_element_type=F32)
        eps = eps.reshape(size, patches, features)
        state = start_v[c] + prefix_v[n].reshape(size, patches, features)
        coef = [coef_v[i][:1, :1].reshape(1, 1, 1) for i in range(7)]
        clean = jnp.clip((state - coef[0] * eps) * coef[1], -1.0, 1.0)
        implied = (state - coef[2] * clean) * coef[3]
        drift = coef[4] * clean + coef[5] * implied + coef[6] * noise_v[c] - state
        drift_v[n] = drift.reshape(2, half, patches, features)
        core_copy(n).start()

    def step(n, carry):
        @pl.when(n >= chunks)
        def _():
            finish(n - chunks)

        compute(n)

        @pl.when(n >= 1)
        def _():
            chain(n - 1)

        @pl.when(n >= chunks - 1)
        def _():
            hand_back(n - chunks + 1)

        return carry

    lax.fori_loop(0, messages, step, 0)

    def emit(m):
        finish(m)
        c = m - (ITERS - 1) * chunks
        whole = prefix_v[m + chunks] + drift_v[m]
        out_v[c] = start_v[c] + whole.reshape(size, patches, features)
        out_copy(c).start()

    chain(messages - 1)
    for m in range(messages - chunks + 1, messages):
        hand_back(m)
        emit(m - 1)
    emit(messages - 1)

    for j in range(1, window):
        gap_copy(j).wait_send()
    for m in range(messages):
        core_copy(m).wait_send()
        final_copy(m).wait_send()
        if columns == 2:
            side_copy(m, chain_tx).wait_send()

    @pl.when(z < rows - 1)
    def _():
        for m in range(messages):
            chain_copy(m).wait_send()

    for c in range(chunks):
        out_copy(c).wait()


def shards(
    steps,
    inner,
    start_state,
    noise_draws,
    step_gaps,
    window_start,
    input_weight,
    embed_weight,
    first_weight,
    second_weight,
    output_weight,
):
    batch, patches, features = start_state.shape
    channels = input_weight.shape[1]
    size = CHUNK_IMAGES
    half, chunks = size // 2, batch // size
    columns = 2 if steps % 2 == 0 else 1
    window = steps * inner
    messages = ITERS * chunks
    chunked = (chunks, size, patches, features)
    piece = (messages, half, patches, features)
    cfg = (steps, inner, columns, chunks, size, patches, features, channels)
    table = jnp.asarray(noise_table())
    freq = jnp.asarray(frequencies(embed_weight.shape[0] // 2))
    matrix = jnp.asarray(group_matrix(channels, patches)).astype(BF16)
    smem = pl.BlockSpec(memory_space=pltpu.SMEM)
    vmem = pl.BlockSpec(memory_space=pltpu.VMEM)
    anywhere = pl.BlockSpec(memory_space=pl.ANY)
    dma = pltpu.SemaphoreType.DMA
    out = pl.pallas_call(
        functools.partial(kernel, cfg),
        out_shape=jax.ShapeDtypeStruct(chunked, F32),
        in_specs=[smem, smem, vmem, vmem, vmem] + [anywhere] * 7,
        out_specs=anywhere,
        scratch_shapes=[
            pltpu.VMEM(chunked, F32),
            pltpu.VMEM(chunked, F32),
            pltpu.VMEM(input_weight.shape, BF16),
            pltpu.VMEM(embed_weight.shape, BF16),
            pltpu.VMEM(first_weight.shape, BF16),
            pltpu.VMEM(second_weight.shape, BF16),
            pltpu.VMEM(output_weight.shape, BF16),
            pltpu.VMEM((8, LANES), jnp.int32),
            pltpu.VMEM((window, 8, LANES), jnp.int32),
            pltpu.VMEM((8, 2 * channels), F32),
            pltpu.VMEM((7, 8, LANES), F32),
            pltpu.VMEM((messages, 2, half, patches, features), F32),
            pltpu.VMEM(piece, F32),
            pltpu.VMEM(piece, F32),
            pltpu.VMEM(piece, F32),
            pltpu.VMEM(piece, F32),
            pltpu.VMEM(piece, F32),
            pltpu.VMEM((messages + chunks, 2, half, patches, features), F32),
            pltpu.VMEM(chunked, F32),
            dma((7,)),
            dma((window,)),
            dma((window,)),
        ]
        + [dma((messages,))] * 8
        + [dma((chunks,))],
        compiler_params=pltpu.CompilerParams(
            collective_id=0, has_side_effects=True, vmem_limit_bytes=56 * 1024 * 1024
        ),
    )(
        step_gaps,
        window_start,
        table,
        freq,
        matrix,
        start_state.reshape(chunked),
        noise_draws.reshape(chunked),
        input_weight,
        embed_weight,
        first_weight,
        second_weight,
        output_weight,
    )
    return out.reshape((1,) + start_state.shape)


def solution(mesh):
    steps, inner = mesh.shape["steps"], mesh.shape["inner"]
    return jax.shard_map(
        functools.partial(shards, steps, inner),
        mesh=mesh,
        in_specs=(
            P("groups", None, None),
            P(("groups", "steps", "inner"), None, None, None),
            P(("groups", "steps", "inner")),
            P("groups"),
            P(),
            P(),
            P(),
            P(),
            P(),
        ),
        out_specs=P(("groups", "steps", "inner"), None, None, None),
        check_vma=False,
    )
```

```python
import functools
import math

import jax
import jax.numpy as jnp
import numpy as np
from jax import lax
from jax.experimental import pallas as pl
from jax.experimental.pallas import tpu as pltpu
from jax.sharding import PartitionSpec as P

GROUPS = 32
PIECES = 2
ITERS = 2
TRAIN_STEPS = 1000
CHUNK_IMAGES = 2
LANES = 128
BLOCK = 256
MESH = pl.DeviceIdType.MESH
F32 = jnp.float32
BF16 = jnp.bfloat16


def noise_table():
    levels = np.arange(TRAIN_STEPS, dtype=np.float32)
    beta = (0.0001 + (0.02 - 0.0001) * levels / (TRAIN_STEPS - 1)).astype(np.float32)
    bars = np.exp(np.cumsum(np.log1p(-beta.astype(np.float64)))).astype(np.float32)
    padded = np.zeros((-(-TRAIN_STEPS // (8 * LANES)) * 8 * LANES,), np.float32)
    padded[:TRAIN_STEPS] = bars
    return padded.reshape(-1, LANES)


def frequencies(count):
    powers = -math.log(10000.0) * np.arange(count, dtype=np.float32) / count
    return np.exp(powers.astype(np.float32)).astype(np.float32)[None, :]


def group_matrix(channels, rows):
    width = channels // GROUPS
    place = np.arange(BLOCK) // width
    same = (place[:, None] == place[None, :]).astype(np.float32)
    return same / (width * rows)


def silu(value):
    half = 0.5 * value
    return half + half * jnp.tanh(half)


def kernel(
    cfg,
    gap_ref,
    start_level_ref,
    table_ref,
    freq_ref,
    group_ref,
    start_hbm,
    noise_hbm,
    win_hbm,
    wemb_hbm,
    w1_hbm,
    w2_hbm,
    wout_hbm,
    out_v,
    start_v,
    noise_v,
    win,
    wemb,
    w1,
    w2,
    wout,
    gap_send,
    gap_all,
    modulation_v,
    coef_v,
    drift_v,
    core_rx,
    chain_rx,
    chain_tx,
    side_rx,
    final_tx,
    prefix_v,
    load_sem,
    gap_send_sem,
    gap_recv_sem,
    core_send,
    core_recv,
    chain_send,
    chain_recv,
    side_send,
    side_recv,
    final_send,
    final_recv,
):
    steps, inner, columns, chunks, size, patches, features, channels = cfg
    rows = steps // columns
    half = size // 2
    total = size * patches
    s = lax.axis_index("steps")
    h = lax.axis_index("inner")
    z, y = s // columns, lax.rem(s, columns)
    window = steps * inner
    me = s * inner + h
    messages = ITERS * chunks

    loads = [
        pltpu.make_async_copy(src, dst, load_sem.at[i])
        for i, (src, dst) in enumerate(
            [
                (start_hbm, start_v),
                (win_hbm, win),
                (wemb_hbm, wemb),
                (w1_hbm, w1),
                (w2_hbm, w2),
                (wout_hbm, wout),
                (noise_hbm, noise_v),
            ]
        )
    ]
    for load in loads:
        load.start()
    gap_send[...] = jnp.zeros_like(gap_send) + gap_ref[0]

    barrier = pltpu.get_barrier_semaphore()
    for j in range(1, window):
        to = lax.rem(me + j, window)
        pl.semaphore_signal(
            barrier,
            inc=1,
            device_id={"steps": to // inner, "inner": lax.rem(to, inner)},
            device_id_type=MESH,
        )
    pl.semaphore_wait(barrier, window - 1)

    def gap_copy(j):
        to = lax.rem(me + j, window)
        return pltpu.make_async_remote_copy(
            src_ref=gap_send,
            dst_ref=gap_all.at[me],
            send_sem=gap_send_sem.at[j],
            recv_sem=gap_recv_sem.at[me],
            device_id={"steps": to // inner, "inner": lax.rem(to, inner)},
            device_id_type=MESH,
        )

    def gap_arrival(j):
        origin = lax.rem(me + j, window)
        return pltpu.make_async_remote_copy(
            src_ref=gap_send,
            dst_ref=gap_all.at[origin],
            send_sem=gap_send_sem.at[j],
            recv_sem=gap_recv_sem.at[origin],
            device_id={"steps": origin // inner, "inner": lax.rem(origin, inner)},
            device_id_type=MESH,
        )

    for j in range(1, window):
        gap_copy(j).start()

    for n in range(chunks):
        prefix_v[n] = jnp.zeros(prefix_v.shape[1:], F32)

    @pl.when(z == 0)
    def _():
        chain_rx[...] = jnp.zeros_like(chain_rx)

    def core_copy(m):
        return pltpu.make_async_remote_copy(
            src_ref=drift_v.at[m, 1 - h],
            dst_ref=core_rx.at[m],
            send_sem=core_send.at[m],
            recv_sem=core_recv.at[m],
            device_id={"inner": 1 - h},
            device_id_type=MESH,
        )

    depth = patches // PIECES

    def part(ref, m, q):
        return ref.at[m, :, q * depth : (q + 1) * depth]

    def chain_copy(m, q):
        return pltpu.make_async_remote_copy(
            src_ref=part(chain_tx, m, q),
            dst_ref=part(chain_rx, m, q),
            send_sem=chain_send.at[m, q],
            recv_sem=chain_recv.at[m, q],
            device_id={"steps": lax.rem(s + columns, steps)},
            device_id_type=MESH,
        )

    def side_copy(m, source, q):
        return pltpu.make_async_remote_copy(
            src_ref=part(source, m, q),
            dst_ref=part(side_rx, m, q),
            send_sem=side_send.at[m, q],
            recv_sem=side_recv.at[m, q],
            device_id={"steps": z * columns + (1 - y)},
            device_id_type=MESH,
        )

    def final_copy(m):
        return pltpu.make_async_remote_copy(
            src_ref=final_tx.at[m],
            dst_ref=prefix_v.at[m + chunks, h],
            send_sem=final_send.at[m],
            recv_sem=final_recv.at[m],
            device_id={"inner": 1 - h},
            device_id_type=MESH,
        )

    def final_arrival(m):
        return pltpu.make_async_remote_copy(
            src_ref=final_tx.at[m],
            dst_ref=prefix_v.at[m + chunks, 1 - h],
            send_sem=final_send.at[m],
            recv_sem=final_recv.at[m],
            device_id={"inner": 1 - h},
            device_id_type=MESH,
        )

    def chain(m):
        core_copy(m).wait_recv()
        for q in range(PIECES):
            cut = slice(q * depth, (q + 1) * depth)

            @pl.when(z > 0)
            def _():
                chain_copy(m, q).wait_recv()

            chain_tx[m, :, cut] = chain_rx[m, :, cut] + (drift_v[m, h, :, cut] + core_rx[m, :, cut])

            @pl.when(z < rows - 1)
            def _():
                chain_copy(m, q).start()

            if columns == 2:

                @pl.when(y == 0)
                def _():
                    side_copy(m, chain_tx, q).start()

                @pl.when(y == 1)
                def _():
                    side_copy(m, chain_rx, q).start()

    def hand_back(m):
        prefix = chain_rx[m]
        if columns == 2:
            for q in range(PIECES):
                side_copy(m, chain_tx, q).wait_recv()
            prefix = prefix + side_rx[m]

        @pl.when(h == 0)
        def _():
            final_tx[m] = prefix + drift_v[m, 0]
            prefix_v[m + chunks, 0] = prefix

        @pl.when(h == 1)
        def _():
            final_tx[m] = prefix
            prefix_v[m + chunks, 1] = prefix + core_rx[m]

        final_copy(m).start()

    def finish(m):
        final_arrival(m).wait_recv()

    def group_average(partial):
        blocks = channels // BLOCK
        stacked = jnp.concatenate(
            [partial[:, i * BLOCK : (i + 1) * BLOCK] for i in range(blocks)], axis=0
        )
        matrix = group_ref[...]
        high = stacked.astype(BF16)
        rest = stacked - high.astype(F32)
        middle = rest.astype(BF16)
        low = (rest - middle.astype(F32)).astype(BF16)
        summed = (
            jnp.dot(low, matrix, preferred_element_type=F32)
            + jnp.dot(middle, matrix, preferred_element_type=F32)
            + jnp.dot(high, matrix, preferred_element_type=F32)
        )
        summed = jnp.sum(summed.reshape(blocks, size, 8, BLOCK), axis=2, keepdims=True)
        return jnp.concatenate([summed[i] for i in range(blocks)], axis=-1)

    def row_sums(value):
        return jnp.sum(value.reshape(size, patches // 8, 8, channels), axis=1).reshape(
            size * 8, channels
        )

    def centered(hidden):
        shaped = hidden.reshape(size, patches, channels)
        offset = shaped - group_average(row_sums(shaped))
        return offset, lax.rsqrt(group_average(row_sums(offset * offset)) + 1e-05)

    def set_level():
        for j in range(1, window):
            gap_arrival(j).wait_recv()
        earlier = jnp.zeros(gap_send.shape, jnp.int32)
        for k in range(window):
            earlier = earlier + jnp.where(k < me, gap_all[k], 0)
        level_now = start_level_ref[0] - earlier
        level_next = level_now - gap_ref[0]
        table = table_ref[...]
        places = lax.broadcasted_iota(jnp.int32, table.shape, 0) * LANES + (
            lax.broadcasted_iota(jnp.int32, table.shape, 1)
        )

        def lookup(level):
            found = jnp.where(places == level[:1, :1], table, 0.0)
            return jnp.sum(jnp.sum(found, axis=0, keepdims=True), axis=1, keepdims=True)

        bar_now, bar_next = lookup(level_now), lookup(level_next)
        coefs = [
            jnp.sqrt(1.0 - bar_now),
            1.0 / jnp.sqrt(bar_now),
            jnp.sqrt(bar_now),
            1.0 / jnp.sqrt(1.0 - bar_now),
            jnp.sqrt(bar_next),
            (1.0 - bar_next) * jnp.sqrt(bar_now / (bar_next * (1.0 - bar_now))),
            jnp.sqrt((1.0 - bar_next) / (1.0 - bar_now) * (1.0 - bar_now / bar_next)),
        ]
        for i, coef in enumerate(coefs):
            coef_v[i] = jnp.broadcast_to(coef, coef_v.shape[1:])
        angles = level_now.astype(F32)[:, :1] * freq_ref[...]
        around = jnp.concatenate([jnp.cos(angles), jnp.sin(angles)], axis=1).astype(BF16)
        loads[2].wait()
        modulation_v[...] = jnp.dot(around, wemb[...], preferred_element_type=F32)

    def compute(n):
        c = lax.rem(n, chunks)

        state = start_v[c] + prefix_v[n].reshape(size, patches, features)
        flat = state.reshape(total, features).astype(BF16)
        entry = jnp.dot(flat, win[...], preferred_element_type=F32)
        offset, spread = centered(entry)

        scale = modulation_v[:1, :channels].reshape(1, 1, channels)
        shift = modulation_v[:1, channels:].reshape(1, 1, channels)
        one = silu(offset * (spread * (1.0 + scale)) + shift).astype(BF16)
        middle = jnp.dot(one.reshape(total, channels), w1[...], preferred_element_type=F32)
        offset, spread = centered(middle)
        two = silu(offset * spread).astype(BF16)

        @pl.when(n >= chunks - 1)
        def _():
            hand_back(n - chunks + 1)

        block = entry + jnp.dot(
            two.reshape(total, channels), w2[...], preferred_element_type=F32
        )
        offset, spread = centered(block)
        three = silu(offset * spread).astype(BF16)

        eps = jnp.dot(three.reshape(total, channels), wout[...], preferred_element_type=F32)
        eps = eps.reshape(size, patches, features)
        state = start_v[c] + prefix_v[n].reshape(size, patches, features)
        coef = [coef_v[i][:1, :1].reshape(1, 1, 1) for i in range(7)]
        clean = jnp.clip((state - coef[0] * eps) * coef[1], -1.0, 1.0)
        implied = (state - coef[2] * clean) * coef[3]
        drift = coef[4] * clean + coef[5] * implied + coef[6] * noise_v[c] - state
        drift_v[n] = drift.reshape(2, half, patches, features)
        core_copy(n).start()

    def step(n, carry):
        @pl.when(n >= chunks)
        def _():
            finish(n - chunks)

        compute(n)

        @pl.when(n >= 1)
        def _():
            chain(n - 1)

        return carry

    for i in (0, 1, 3, 4, 5, 6):
        loads[i].wait()
    set_level()
    lax.fori_loop(0, messages, step, 0)

    def emit(m):
        finish(m)
        c = m - (ITERS - 1) * chunks
        whole = prefix_v[m + chunks] + drift_v[m]
        out_v[c] = start_v[c] + whole.reshape(size, patches, features)

    chain(messages - 1)
    for m in range(messages - chunks + 1, messages):
        hand_back(m)
        emit(m - 1)
    emit(messages - 1)

    for j in range(1, window):
        gap_copy(j).wait_send()
    for m in range(messages):
        core_copy(m).wait_send()
        final_copy(m).wait_send()
        if columns == 2:
            for q in range(PIECES):
                side_copy(m, chain_tx, q).wait_send()

    @pl.when(z < rows - 1)
    def _():
        for m in range(messages):
            for q in range(PIECES):
                chain_copy(m, q).wait_send()


def shards(
    steps,
    inner,
    start_state,
    noise_draws,
    step_gaps,
    window_start,
    input_weight,
    embed_weight,
    first_weight,
    second_weight,
    output_weight,
):
    batch, patches, features = start_state.shape
    channels = input_weight.shape[1]
    size = CHUNK_IMAGES
    half, chunks = size // 2, batch // size
    columns = 2 if steps % 2 == 0 else 1
    window = steps * inner
    messages = ITERS * chunks
    chunked = (chunks, size, patches, features)
    piece = (messages, half, patches, features)
    cfg = (steps, inner, columns, chunks, size, patches, features, channels)
    table = jnp.asarray(noise_table())
    freq = jnp.asarray(frequencies(embed_weight.shape[0] // 2))
    matrix = jnp.asarray(group_matrix(channels, patches)).astype(BF16)
    smem = pl.BlockSpec(memory_space=pltpu.SMEM)
    vmem = pl.BlockSpec(memory_space=pltpu.VMEM)
    anywhere = pl.BlockSpec(memory_space=pltpu.HBM)
    dma = pltpu.SemaphoreType.DMA
    out = pl.pallas_call(
        functools.partial(kernel, cfg),
        out_shape=pltpu.VMEM(chunked, F32),
        in_specs=[smem, smem, vmem, vmem, vmem] + [anywhere] * 7,
        out_specs=vmem,
        scratch_shapes=[
            pltpu.VMEM(chunked, F32),
            pltpu.VMEM(chunked, F32),
            pltpu.VMEM(input_weight.shape, BF16),
            pltpu.VMEM(embed_weight.shape, BF16),
            pltpu.VMEM(first_weight.shape, BF16),
            pltpu.VMEM(second_weight.shape, BF16),
            pltpu.VMEM(output_weight.shape, BF16),
            pltpu.VMEM((8, LANES), jnp.int32),
            pltpu.VMEM((window, 8, LANES), jnp.int32),
            pltpu.VMEM((8, 2 * channels), F32),
            pltpu.VMEM((7, 8, LANES), F32),
            pltpu.VMEM((messages, 2, half, patches, features), F32),
            pltpu.VMEM(piece, F32),
            pltpu.VMEM(piece, F32),
            pltpu.VMEM(piece, F32),
            pltpu.VMEM(piece, F32),
            pltpu.VMEM(piece, F32),
            pltpu.VMEM((messages + chunks, 2, half, patches, features), F32),
            dma((7,)),
            dma((window,)),
            dma((window,)),
        ]
        + [dma((messages,))] * 2
        + [dma((messages, PIECES))] * 4
        + [dma((messages,))] * 2,
        compiler_params=pltpu.CompilerParams(
            collective_id=0, has_side_effects=True, vmem_limit_bytes=56 * 1024 * 1024
        ),
    )(
        step_gaps,
        window_start,
        table,
        freq,
        matrix,
        start_state.reshape(chunked),
        noise_draws.reshape(chunked),
        input_weight,
        embed_weight,
        first_weight,
        second_weight,
        output_weight,
    )
    return out.reshape((1,) + start_state.shape)


def solution(mesh):
    steps, inner = mesh.shape["steps"], mesh.shape["inner"]
    return jax.shard_map(
        functools.partial(shards, steps, inner),
        mesh=mesh,
        in_specs=(
            P("groups", None, None),
            P(("groups", "steps", "inner"), None, None, None),
            P(("groups", "steps", "inner")),
            P("groups"),
            P(),
            P(),
            P(),
            P(),
            P(),
        ),
        out_specs=P(("groups", "steps", "inner"), None, None, None),
        check_vma=False,
    )
```

```python
import functools
import math

import jax
import jax.numpy as jnp
import numpy as np
from jax import lax
from jax.experimental import pallas as pl
from jax.experimental.pallas import tpu as pltpu
from jax.sharding import PartitionSpec as P

GROUPS = 32
PIECES = 4
ITERS = 2
TRAIN_STEPS = 1000
CHUNK_IMAGES = 2
LANES = 128
BLOCK = 256
MESH = pl.DeviceIdType.MESH
F32 = jnp.float32
BF16 = jnp.bfloat16


def noise_table():
    levels = np.arange(TRAIN_STEPS, dtype=np.float32)
    beta = (0.0001 + (0.02 - 0.0001) * levels / (TRAIN_STEPS - 1)).astype(np.float32)
    bars = np.exp(np.cumsum(np.log1p(-beta.astype(np.float64)))).astype(np.float32)
    padded = np.zeros((-(-TRAIN_STEPS // (8 * LANES)) * 8 * LANES,), np.float32)
    padded[:TRAIN_STEPS] = bars
    return padded.reshape(-1, LANES)


def frequencies(count):
    powers = -math.log(10000.0) * np.arange(count, dtype=np.float32) / count
    return np.exp(powers.astype(np.float32)).astype(np.float32)[None, :]


def group_matrix(channels, rows):
    width = channels // GROUPS
    place = np.arange(BLOCK) // width
    same = (place[:, None] == place[None, :]).astype(np.float32)
    return same / (width * rows)


def silu(value):
    half = 0.5 * value
    return half + half * jnp.tanh(half)


def kernel(
    cfg,
    gap_ref,
    start_level_ref,
    table_ref,
    freq_ref,
    group_ref,
    start_hbm,
    noise_hbm,
    win_hbm,
    wemb_hbm,
    w1_hbm,
    w2_hbm,
    wout_hbm,
    out_v,
    start_v,
    noise_v,
    win,
    wemb,
    w1,
    w2,
    wout,
    gap_send,
    gap_all,
    modulation_v,
    coef_v,
    drift_v,
    core_rx,
    chain_rx,
    chain_tx,
    side_rx,
    final_tx,
    prefix_v,
    load_sem,
    gap_send_sem,
    gap_recv_sem,
    core_send,
    core_recv,
    chain_send,
    chain_recv,
    side_send,
    side_recv,
    final_send,
    final_recv,
):
    steps, inner, columns, chunks, size, patches, features, channels = cfg
    rows = steps // columns
    half = size // 2
    total = size * patches
    s = lax.axis_index("steps")
    h = lax.axis_index("inner")
    z, y = s // columns, lax.rem(s, columns)
    window = steps * inner
    me = s * inner + h
    messages = ITERS * chunks

    loads = [
        pltpu.make_async_copy(src, dst, load_sem.at[i])
        for i, (src, dst) in enumerate(
            [
                (start_hbm, start_v),
                (win_hbm, win),
                (wemb_hbm, wemb),
                (w1_hbm, w1),
                (w2_hbm, w2),
                (wout_hbm, wout),
                (noise_hbm, noise_v),
            ]
        )
    ]
    for load in loads:
        load.start()
    gap_send[...] = jnp.zeros_like(gap_send) + gap_ref[0]

    barrier = pltpu.get_barrier_semaphore()
    for j in range(1, window):
        to = lax.rem(me + j, window)
        pl.semaphore_signal(
            barrier,
            inc=1,
            device_id={"steps": to // inner, "inner": lax.rem(to, inner)},
            device_id_type=MESH,
        )
    pl.semaphore_wait(barrier, window - 1)

    def gap_copy(j):
        to = lax.rem(me + j, window)
        return pltpu.make_async_remote_copy(
            src_ref=gap_send,
            dst_ref=gap_all.at[me],
            send_sem=gap_send_sem.at[j],
            recv_sem=gap_recv_sem.at[me],
            device_id={"steps": to // inner, "inner": lax.rem(to, inner)},
            device_id_type=MESH,
        )

    def gap_arrival(j):
        origin = lax.rem(me + j, window)
        return pltpu.make_async_remote_copy(
            src_ref=gap_send,
            dst_ref=gap_all.at[origin],
            send_sem=gap_send_sem.at[j],
            recv_sem=gap_recv_sem.at[origin],
            device_id={"steps": origin // inner, "inner": lax.rem(origin, inner)},
            device_id_type=MESH,
        )

    for j in range(1, window):
        gap_copy(j).start()

    for n in range(chunks):
        prefix_v[n] = jnp.zeros(prefix_v.shape[1:], F32)

    @pl.when(z == 0)
    def _():
        chain_rx[...] = jnp.zeros_like(chain_rx)

    def core_copy(m):
        return pltpu.make_async_remote_copy(
            src_ref=drift_v.at[m, 1 - h],
            dst_ref=core_rx.at[m],
            send_sem=core_send.at[m],
            recv_sem=core_recv.at[m],
            device_id={"inner": 1 - h},
            device_id_type=MESH,
        )

    depth = patches // PIECES

    def part(ref, m, q):
        return ref.at[m, :, q * depth : (q + 1) * depth]

    def chain_copy(m, q):
        return pltpu.make_async_remote_copy(
            src_ref=part(chain_tx, m, q),
            dst_ref=part(chain_rx, m, q),
            send_sem=chain_send.at[m, q],
            recv_sem=chain_recv.at[m, q],
            device_id={"steps": lax.rem(s + columns, steps)},
            device_id_type=MESH,
        )

    def side_copy(m, source, q):
        return pltpu.make_async_remote_copy(
            src_ref=part(source, m, q),
            dst_ref=part(side_rx, m, q),
            send_sem=side_send.at[m, q],
            recv_sem=side_recv.at[m, q],
            device_id={"steps": z * columns + (1 - y)},
            device_id_type=MESH,
        )

    def final_copy(m):
        return pltpu.make_async_remote_copy(
            src_ref=final_tx.at[m],
            dst_ref=prefix_v.at[m + chunks, h],
            send_sem=final_send.at[m],
            recv_sem=final_recv.at[m],
            device_id={"inner": 1 - h},
            device_id_type=MESH,
        )

    def final_arrival(m):
        return pltpu.make_async_remote_copy(
            src_ref=final_tx.at[m],
            dst_ref=prefix_v.at[m + chunks, 1 - h],
            send_sem=final_send.at[m],
            recv_sem=final_recv.at[m],
            device_id={"inner": 1 - h},
            device_id_type=MESH,
        )

    def chain(m):
        core_copy(m).wait_recv()
        for q in range(PIECES):
            cut = slice(q * depth, (q + 1) * depth)

            @pl.when(z > 0)
            def _():
                chain_copy(m, q).wait_recv()

            chain_tx[m, :, cut] = chain_rx[m, :, cut] + (drift_v[m, h, :, cut] + core_rx[m, :, cut])

            @pl.when(z < rows - 1)
            def _():
                chain_copy(m, q).start()

            if columns == 2:

                @pl.when(y == 0)
                def _():
                    side_copy(m, chain_tx, q).start()

                @pl.when(y == 1)
                def _():
                    side_copy(m, chain_rx, q).start()

    def hand_back(m):
        prefix = chain_rx[m]
        if columns == 2:
            for q in range(PIECES):
                side_copy(m, chain_tx, q).wait_recv()
            prefix = prefix + side_rx[m]

        @pl.when(h == 0)
        def _():
            final_tx[m] = prefix + drift_v[m, 0]
            prefix_v[m + chunks, 0] = prefix

        @pl.when(h == 1)
        def _():
            final_tx[m] = prefix
            prefix_v[m + chunks, 1] = prefix + core_rx[m]

        final_copy(m).start()

    def finish(m):
        final_arrival(m).wait_recv()

    def group_average(partial):
        blocks = channels // BLOCK
        stacked = jnp.concatenate(
            [partial[:, i * BLOCK : (i + 1) * BLOCK] for i in range(blocks)], axis=0
        )
        matrix = group_ref[...]
        high = stacked.astype(BF16)
        rest = stacked - high.astype(F32)
        middle = rest.astype(BF16)
        low = (rest - middle.astype(F32)).astype(BF16)
        summed = (
            jnp.dot(low, matrix, preferred_element_type=F32)
            + jnp.dot(middle, matrix, preferred_element_type=F32)
            + jnp.dot(high, matrix, preferred_element_type=F32)
        )
        summed = jnp.sum(summed.reshape(blocks, size, 8, BLOCK), axis=2, keepdims=True)
        return jnp.concatenate([summed[i] for i in range(blocks)], axis=-1)

    def row_sums(value):
        return jnp.sum(value.reshape(size, patches // 8, 8, channels), axis=1).reshape(
            size * 8, channels
        )

    def centered(hidden):
        shaped = hidden.reshape(size, patches, channels)
        offset = shaped - group_average(row_sums(shaped))
        return offset, lax.rsqrt(group_average(row_sums(offset * offset)) + 1e-05)

    def set_level():
        for j in range(1, window):
            gap_arrival(j).wait_recv()
        earlier = jnp.zeros(gap_send.shape, jnp.int32)
        for k in range(window):
            earlier = earlier + jnp.where(k < me, gap_all[k], 0)
        level_now = start_level_ref[0] - earlier
        level_next = level_now - gap_ref[0]
        table = table_ref[...]
        places = lax.broadcasted_iota(jnp.int32, table.shape, 0) * LANES + (
            lax.broadcasted_iota(jnp.int32, table.shape, 1)
        )

        def lookup(level):
            found = jnp.where(places == level[:1, :1], table, 0.0)
            return jnp.sum(jnp.sum(found, axis=0, keepdims=True), axis=1, keepdims=True)

        bar_now, bar_next = lookup(level_now), lookup(level_next)
        coefs = [
            jnp.sqrt(1.0 - bar_now),
            1.0 / jnp.sqrt(bar_now),
            jnp.sqrt(bar_now),
            1.0 / jnp.sqrt(1.0 - bar_now),
            jnp.sqrt(bar_next),
            (1.0 - bar_next) * jnp.sqrt(bar_now / (bar_next * (1.0 - bar_now))),
            jnp.sqrt((1.0 - bar_next) / (1.0 - bar_now) * (1.0 - bar_now / bar_next)),
        ]
        for i, coef in enumerate(coefs):
            coef_v[i] = jnp.broadcast_to(coef, coef_v.shape[1:])
        angles = level_now.astype(F32)[:, :1] * freq_ref[...]
        around = jnp.concatenate([jnp.cos(angles), jnp.sin(angles)], axis=1).astype(BF16)
        loads[2].wait()
        modulation_v[...] = jnp.dot(around, wemb[...], preferred_element_type=F32)

    def compute(n):
        c = lax.rem(n, chunks)

        state = start_v[c] + prefix_v[n].reshape(size, patches, features)
        flat = state.reshape(total, features).astype(BF16)
        entry = jnp.dot(flat, win[...], preferred_element_type=F32)
        offset, spread = centered(entry)

        scale = modulation_v[:1, :channels].reshape(1, 1, channels)
        shift = modulation_v[:1, channels:].reshape(1, 1, channels)
        one = silu(offset * (spread * (1.0 + scale)) + shift).astype(BF16)
        middle = jnp.dot(one.reshape(total, channels), w1[...], preferred_element_type=F32)
        offset, spread = centered(middle)
        two = silu(offset * spread).astype(BF16)

        @pl.when(n >= chunks - 1)
        def _():
            hand_back(n - chunks + 1)

        block = entry + jnp.dot(
            two.reshape(total, channels), w2[...], preferred_element_type=F32
        )
        offset, spread = centered(block)
        three = silu(offset * spread).astype(BF16)

        eps = jnp.dot(three.reshape(total, channels), wout[...], preferred_element_type=F32)
        eps = eps.reshape(size, patches, features)
        state = start_v[c] + prefix_v[n].reshape(size, patches, features)
        coef = [coef_v[i][:1, :1].reshape(1, 1, 1) for i in range(7)]
        clean = jnp.clip((state - coef[0] * eps) * coef[1], -1.0, 1.0)
        implied = (state - coef[2] * clean) * coef[3]
        drift = coef[4] * clean + coef[5] * implied + coef[6] * noise_v[c] - state
        drift_v[n] = drift.reshape(2, half, patches, features)
        core_copy(n).start()

    def step(n, carry):
        @pl.when(n >= chunks)
        def _():
            finish(n - chunks)

        compute(n)

        @pl.when(n >= 1)
        def _():
            chain(n - 1)

        return carry

    for i in (0, 1, 3, 4, 5, 6):
        loads[i].wait()
    set_level()
    lax.fori_loop(0, messages, step, 0)

    def emit(m):
        finish(m)
        c = m - (ITERS - 1) * chunks
        whole = prefix_v[m + chunks] + drift_v[m]
        out_v[c] = start_v[c] + whole.reshape(size, patches, features)

    chain(messages - 1)
    for m in range(messages - chunks + 1, messages):
        hand_back(m)
        emit(m - 1)
    emit(messages - 1)

    for j in range(1, window):
        gap_copy(j).wait_send()
    for m in range(messages):
        core_copy(m).wait_send()
        final_copy(m).wait_send()
        if columns == 2:
            for q in range(PIECES):
                side_copy(m, chain_tx, q).wait_send()

    @pl.when(z < rows - 1)
    def _():
        for m in range(messages):
            for q in range(PIECES):
                chain_copy(m, q).wait_send()


def shards(
    steps,
    inner,
    start_state,
    noise_draws,
    step_gaps,
    window_start,
    input_weight,
    embed_weight,
    first_weight,
    second_weight,
    output_weight,
):
    batch, patches, features = start_state.shape
    channels = input_weight.shape[1]
    size = CHUNK_IMAGES
    half, chunks = size // 2, batch // size
    columns = 2 if steps % 2 == 0 else 1
    window = steps * inner
    messages = ITERS * chunks
    chunked = (chunks, size, patches, features)
    piece = (messages, half, patches, features)
    cfg = (steps, inner, columns, chunks, size, patches, features, channels)
    table = jnp.asarray(noise_table())
    freq = jnp.asarray(frequencies(embed_weight.shape[0] // 2))
    matrix = jnp.asarray(group_matrix(channels, patches)).astype(BF16)
    smem = pl.BlockSpec(memory_space=pltpu.SMEM)
    vmem = pl.BlockSpec(memory_space=pltpu.VMEM)
    anywhere = pl.BlockSpec(memory_space=pltpu.HBM)
    dma = pltpu.SemaphoreType.DMA
    out = pl.pallas_call(
        functools.partial(kernel, cfg),
        out_shape=pltpu.VMEM(chunked, F32),
        in_specs=[smem, smem, vmem, vmem, vmem] + [anywhere] * 7,
        out_specs=vmem,
        scratch_shapes=[
            pltpu.VMEM(chunked, F32),
            pltpu.VMEM(chunked, F32),
            pltpu.VMEM(input_weight.shape, BF16),
            pltpu.VMEM(embed_weight.shape, BF16),
            pltpu.VMEM(first_weight.shape, BF16),
            pltpu.VMEM(second_weight.shape, BF16),
            pltpu.VMEM(output_weight.shape, BF16),
            pltpu.VMEM((8, LANES), jnp.int32),
            pltpu.VMEM((window, 8, LANES), jnp.int32),
            pltpu.VMEM((8, 2 * channels), F32),
            pltpu.VMEM((7, 8, LANES), F32),
            pltpu.VMEM((messages, 2, half, patches, features), F32),
            pltpu.VMEM(piece, F32),
            pltpu.VMEM(piece, F32),
            pltpu.VMEM(piece, F32),
            pltpu.VMEM(piece, F32),
            pltpu.VMEM(piece, F32),
            pltpu.VMEM((messages + chunks, 2, half, patches, features), F32),
            dma((7,)),
            dma((window,)),
            dma((window,)),
        ]
        + [dma((messages,))] * 2
        + [dma((messages, PIECES))] * 4
        + [dma((messages,))] * 2,
        compiler_params=pltpu.CompilerParams(
            collective_id=0, has_side_effects=True, vmem_limit_bytes=56 * 1024 * 1024
        ),
    )(
        step_gaps,
        window_start,
        table,
        freq,
        matrix,
        start_state.reshape(chunked),
        noise_draws.reshape(chunked),
        input_weight,
        embed_weight,
        first_weight,
        second_weight,
        output_weight,
    )
    return out.reshape((1,) + start_state.shape)


def solution(mesh):
    steps, inner = mesh.shape["steps"], mesh.shape["inner"]
    return jax.shard_map(
        functools.partial(shards, steps, inner),
        mesh=mesh,
        in_specs=(
            P("groups", None, None),
            P(("groups", "steps", "inner"), None, None, None),
            P(("groups", "steps", "inner")),
            P("groups"),
            P(),
            P(),
            P(),
            P(),
            P(),
        ),
        out_specs=P(("groups", "steps", "inner"), None, None, None),
        check_vma=False,
    )
```

```python
import functools
import math

import jax
import jax.numpy as jnp
import numpy as np
from jax import lax
from jax.experimental import pallas as pl
from jax.experimental.pallas import tpu as pltpu
from jax.sharding import PartitionSpec as P

GROUPS = 32
PIECES = 2
ITERS = 2
TRAIN_STEPS = 1000
CHUNK_IMAGES = 2
LANES = 128
BLOCK = 256
MESH = pl.DeviceIdType.MESH
F32 = jnp.float32
BF16 = jnp.bfloat16


def noise_table():
    levels = np.arange(TRAIN_STEPS, dtype=np.float32)
    beta = (0.0001 + (0.02 - 0.0001) * levels / (TRAIN_STEPS - 1)).astype(np.float32)
    bars = np.exp(np.cumsum(np.log1p(-beta.astype(np.float64)))).astype(np.float32)
    padded = np.zeros((-(-TRAIN_STEPS // (8 * LANES)) * 8 * LANES,), np.float32)
    padded[:TRAIN_STEPS] = bars
    return padded.reshape(-1, LANES)


def frequencies(count):
    powers = -math.log(10000.0) * np.arange(count, dtype=np.float32) / count
    return np.exp(powers.astype(np.float32)).astype(np.float32)[None, :]


def group_matrix(channels, rows):
    width = channels // GROUPS
    place = np.arange(BLOCK) // width
    same = (place[:, None] == place[None, :]).astype(np.float32)
    return same / (width * rows)


def silu(value):
    half = 0.5 * value
    return half + half * jnp.tanh(half)


def kernel(
    cfg,
    gap_ref,
    start_level_ref,
    table_ref,
    freq_ref,
    group_ref,
    start_hbm,
    noise_hbm,
    win_hbm,
    wemb_hbm,
    w1_hbm,
    w2_hbm,
    wout_hbm,
    out_v,
    start_v,
    noise_v,
    win,
    wemb,
    w1,
    w2,
    wout,
    gap_send,
    gap_all,
    modulation_v,
    coef_v,
    drift_v,
    core_rx,
    chain_rx,
    chain_tx,
    side_rx,
    final_tx,
    prefix_v,
    load_sem,
    gap_send_sem,
    gap_recv_sem,
    core_send,
    core_recv,
    chain_send,
    chain_recv,
    side_send,
    side_recv,
    final_send,
    final_recv,
):
    steps, inner, columns, chunks, size, patches, features, channels = cfg
    rows = steps // columns
    half = size // 2
    total = size * patches
    s = lax.axis_index("steps")
    h = lax.axis_index("inner")
    z, y = s // columns, lax.rem(s, columns)
    window = steps * inner
    me = s * inner + h
    messages = ITERS * chunks

    loads = [
        pltpu.make_async_copy(src, dst, load_sem.at[i])
        for i, (src, dst) in enumerate(
            [
                (start_hbm, start_v),
                (win_hbm, win),
                (wemb_hbm, wemb),
                (w1_hbm, w1),
                (w2_hbm, w2),
                (wout_hbm, wout),
                (noise_hbm, noise_v),
            ]
        )
    ]
    for load in loads:
        load.start()
    gap_send[...] = jnp.zeros_like(gap_send) + gap_ref[0]

    barrier = pltpu.get_barrier_semaphore()
    for j in range(1, window):
        to = lax.rem(me + j, window)
        pl.semaphore_signal(
            barrier,
            inc=1,
            device_id={"steps": to // inner, "inner": lax.rem(to, inner)},
            device_id_type=MESH,
        )
    pl.semaphore_wait(barrier, window - 1)

    def gap_copy(j):
        to = lax.rem(me + j, window)
        return pltpu.make_async_remote_copy(
            src_ref=gap_send,
            dst_ref=gap_all.at[me],
            send_sem=gap_send_sem.at[j],
            recv_sem=gap_recv_sem.at[me],
            device_id={"steps": to // inner, "inner": lax.rem(to, inner)},
            device_id_type=MESH,
        )

    def gap_arrival(j):
        origin = lax.rem(me + j, window)
        return pltpu.make_async_remote_copy(
            src_ref=gap_send,
            dst_ref=gap_all.at[origin],
            send_sem=gap_send_sem.at[j],
            recv_sem=gap_recv_sem.at[origin],
            device_id={"steps": origin // inner, "inner": lax.rem(origin, inner)},
            device_id_type=MESH,
        )

    for j in range(1, window):
        gap_copy(j).start()

    for n in range(chunks):
        prefix_v[n] = jnp.zeros(prefix_v.shape[1:], F32)

    @pl.when(z == 0)
    def _():
        chain_rx[...] = jnp.zeros_like(chain_rx)

    def core_copy(m):
        return pltpu.make_async_remote_copy(
            src_ref=drift_v.at[m, 1 - h],
            dst_ref=core_rx.at[m],
            send_sem=core_send.at[m],
            recv_sem=core_recv.at[m],
            device_id={"inner": 1 - h},
            device_id_type=MESH,
        )

    depth = patches // PIECES

    def part(ref, m, q):
        return ref.at[m, :, q * depth : (q + 1) * depth]

    def chain_copy(m, q):
        return pltpu.make_async_remote_copy(
            src_ref=part(chain_tx, m, q),
            dst_ref=part(chain_rx, m, q),
            send_sem=chain_send.at[m, q],
            recv_sem=chain_recv.at[m, q],
            device_id={"steps": lax.rem(s + columns, steps)},
            device_id_type=MESH,
        )

    def side_copy(m, source, q):
        return pltpu.make_async_remote_copy(
            src_ref=part(source, m, q),
            dst_ref=part(side_rx, m, q),
            send_sem=side_send.at[m, q],
            recv_sem=side_recv.at[m, q],
            device_id={"steps": z * columns + (1 - y)},
            device_id_type=MESH,
        )

    def final_copy(m):
        return pltpu.make_async_remote_copy(
            src_ref=final_tx.at[m],
            dst_ref=prefix_v.at[m + chunks, h],
            send_sem=final_send.at[m],
            recv_sem=final_recv.at[m],
            device_id={"inner": 1 - h},
            device_id_type=MESH,
        )

    def final_arrival(m):
        return pltpu.make_async_remote_copy(
            src_ref=final_tx.at[m],
            dst_ref=prefix_v.at[m + chunks, 1 - h],
            send_sem=final_send.at[m],
            recv_sem=final_recv.at[m],
            device_id={"inner": 1 - h},
            device_id_type=MESH,
        )

    def chain(m):
        core_copy(m).wait_recv()
        for q in range(PIECES):
            cut = slice(q * depth, (q + 1) * depth)

            @pl.when(z > 0)
            def _():
                chain_copy(m, q).wait_recv()

            chain_tx[m, :, cut] = chain_rx[m, :, cut] + (drift_v[m, h, :, cut] + core_rx[m, :, cut])

            @pl.when(z < rows - 1)
            def _():
                chain_copy(m, q).start()

            if columns == 2:

                @pl.when(y == 0)
                def _():
                    side_copy(m, chain_tx, q).start()

                @pl.when(y == 1)
                def _():
                    side_copy(m, chain_rx, q).start()

    def hand_back(m):
        prefix = chain_rx[m]
        if columns == 2:
            for q in range(PIECES):
                side_copy(m, chain_tx, q).wait_recv()
            prefix = prefix + side_rx[m]

        @pl.when(h == 0)
        def _():
            final_tx[m] = prefix + drift_v[m, 0]
            prefix_v[m + chunks, 0] = prefix

        @pl.when(h == 1)
        def _():
            final_tx[m] = prefix
            prefix_v[m + chunks, 1] = prefix + core_rx[m]

        final_copy(m).start()

    def finish(m):
        final_arrival(m).wait_recv()

    def group_average(partial):
        blocks = channels // BLOCK
        stacked = jnp.concatenate(
            [partial[:, i * BLOCK : (i + 1) * BLOCK] for i in range(blocks)], axis=0
        )
        matrix = group_ref[...]
        high = stacked.astype(BF16)
        rest = stacked - high.astype(F32)
        middle = rest.astype(BF16)
        low = (rest - middle.astype(F32)).astype(BF16)
        parts = jnp.concatenate([low, middle, high], axis=0)
        summed = jnp.dot(parts, matrix, preferred_element_type=F32)
        summed = jnp.sum(summed.reshape(3, -1, BLOCK), axis=0)
        summed = jnp.sum(summed.reshape(blocks, size, 8, BLOCK), axis=2, keepdims=True)
        return jnp.concatenate([summed[i] for i in range(blocks)], axis=-1)

    def row_sums(value):
        return jnp.sum(value.reshape(size, patches // 8, 8, channels), axis=1).reshape(
            size * 8, channels
        )

    def centered(hidden):
        shaped = hidden.reshape(size, patches, channels)
        offset = shaped - group_average(row_sums(shaped))
        return offset, lax.rsqrt(group_average(row_sums(offset * offset)) + 1e-05)

    def set_level():
        for j in range(1, window):
            gap_arrival(j).wait_recv()
        earlier = jnp.zeros(gap_send.shape, jnp.int32)
        for k in range(window):
            earlier = earlier + jnp.where(k < me, gap_all[k], 0)
        level_now = start_level_ref[0] - earlier
        level_next = level_now - gap_ref[0]
        table = table_ref[...]
        places = lax.broadcasted_iota(jnp.int32, table.shape, 0) * LANES + (
            lax.broadcasted_iota(jnp.int32, table.shape, 1)
        )

        def lookup(level):
            found = jnp.where(places == level[:1, :1], table, 0.0)
            return jnp.sum(jnp.sum(found, axis=0, keepdims=True), axis=1, keepdims=True)

        bar_now, bar_next = lookup(level_now), lookup(level_next)
        coefs = [
            jnp.sqrt(1.0 - bar_now),
            1.0 / jnp.sqrt(bar_now),
            jnp.sqrt(bar_now),
            1.0 / jnp.sqrt(1.0 - bar_now),
            jnp.sqrt(bar_next),
            (1.0 - bar_next) * jnp.sqrt(bar_now / (bar_next * (1.0 - bar_now))),
            jnp.sqrt((1.0 - bar_next) / (1.0 - bar_now) * (1.0 - bar_now / bar_next)),
        ]
        for i, coef in enumerate(coefs):
            coef_v[i] = jnp.broadcast_to(coef, coef_v.shape[1:])
        angles = level_now.astype(F32)[:, :1] * freq_ref[...]
        around = jnp.concatenate([jnp.cos(angles), jnp.sin(angles)], axis=1).astype(BF16)
        loads[2].wait()
        modulation_v[...] = jnp.dot(around, wemb[...], preferred_element_type=F32)

    def compute(n):
        c = lax.rem(n, chunks)

        state = start_v[c] + prefix_v[n].reshape(size, patches, features)
        flat = state.reshape(total, features).astype(BF16)
        entry = jnp.dot(flat, win[...], preferred_element_type=F32)
        offset, spread = centered(entry)

        scale = modulation_v[:1, :channels].reshape(1, 1, channels)
        shift = modulation_v[:1, channels:].reshape(1, 1, channels)
        one = silu(offset * (spread * (1.0 + scale)) + shift).astype(BF16)
        middle = jnp.dot(one.reshape(total, channels), w1[...], preferred_element_type=F32)
        offset, spread = centered(middle)
        two = silu(offset * spread).astype(BF16)

        @pl.when(n >= chunks - 1)
        def _():
            hand_back(n - chunks + 1)

        block = entry + jnp.dot(
            two.reshape(total, channels), w2[...], preferred_element_type=F32
        )
        offset, spread = centered(block)
        three = silu(offset * spread).astype(BF16)

        eps = jnp.dot(three.reshape(total, channels), wout[...], preferred_element_type=F32)
        eps = eps.reshape(size, patches, features)
        state = start_v[c] + prefix_v[n].reshape(size, patches, features)
        coef = [coef_v[i][:1, :1].reshape(1, 1, 1) for i in range(7)]
        clean = jnp.clip((state - coef[0] * eps) * coef[1], -1.0, 1.0)
        implied = (state - coef[2] * clean) * coef[3]
        drift = coef[4] * clean + coef[5] * implied + coef[6] * noise_v[c] - state
        drift_v[n] = drift.reshape(2, half, patches, features)
        core_copy(n).start()

    def step(n, carry):
        @pl.when(n >= chunks)
        def _():
            finish(n - chunks)

        compute(n)

        @pl.when(n >= 1)
        def _():
            chain(n - 1)

        return carry

    for i in (0, 1, 3, 4, 5, 6):
        loads[i].wait()
    set_level()
    lax.fori_loop(0, messages, step, 0)

    def emit(m):
        finish(m)
        c = m - (ITERS - 1) * chunks
        whole = prefix_v[m + chunks] + drift_v[m]
        out_v[c] = start_v[c] + whole.reshape(size, patches, features)

    chain(messages - 1)
    for m in range(messages - chunks + 1, messages):
        hand_back(m)
        emit(m - 1)
    emit(messages - 1)

    for j in range(1, window):
        gap_copy(j).wait_send()
    for m in range(messages):
        core_copy(m).wait_send()
        final_copy(m).wait_send()
        if columns == 2:
            for q in range(PIECES):
                side_copy(m, chain_tx, q).wait_send()

    @pl.when(z < rows - 1)
    def _():
        for m in range(messages):
            for q in range(PIECES):
                chain_copy(m, q).wait_send()


def shards(
    steps,
    inner,
    start_state,
    noise_draws,
    step_gaps,
    window_start,
    input_weight,
    embed_weight,
    first_weight,
    second_weight,
    output_weight,
):
    batch, patches, features = start_state.shape
    channels = input_weight.shape[1]
    size = CHUNK_IMAGES
    half, chunks = size // 2, batch // size
    columns = 2 if steps % 2 == 0 else 1
    window = steps * inner
    messages = ITERS * chunks
    chunked = (chunks, size, patches, features)
    piece = (messages, half, patches, features)
    cfg = (steps, inner, columns, chunks, size, patches, features, channels)
    table = jnp.asarray(noise_table())
    freq = jnp.asarray(frequencies(embed_weight.shape[0] // 2))
    matrix = jnp.asarray(group_matrix(channels, patches)).astype(BF16)
    smem = pl.BlockSpec(memory_space=pltpu.SMEM)
    vmem = pl.BlockSpec(memory_space=pltpu.VMEM)
    anywhere = pl.BlockSpec(memory_space=pltpu.HBM)
    dma = pltpu.SemaphoreType.DMA
    out = pl.pallas_call(
        functools.partial(kernel, cfg),
        out_shape=pltpu.VMEM(chunked, F32),
        in_specs=[smem, smem, vmem, vmem, vmem] + [anywhere] * 7,
        out_specs=vmem,
        scratch_shapes=[
            pltpu.VMEM(chunked, F32),
            pltpu.VMEM(chunked, F32),
            pltpu.VMEM(input_weight.shape, BF16),
            pltpu.VMEM(embed_weight.shape, BF16),
            pltpu.VMEM(first_weight.shape, BF16),
            pltpu.VMEM(second_weight.shape, BF16),
            pltpu.VMEM(output_weight.shape, BF16),
            pltpu.VMEM((8, LANES), jnp.int32),
            pltpu.VMEM((window, 8, LANES), jnp.int32),
            pltpu.VMEM((8, 2 * channels), F32),
            pltpu.VMEM((7, 8, LANES), F32),
            pltpu.VMEM((messages, 2, half, patches, features), F32),
            pltpu.VMEM(piece, F32),
            pltpu.VMEM(piece, F32),
            pltpu.VMEM(piece, F32),
            pltpu.VMEM(piece, F32),
            pltpu.VMEM(piece, F32),
            pltpu.VMEM((messages + chunks, 2, half, patches, features), F32),
            dma((7,)),
            dma((window,)),
            dma((window,)),
        ]
        + [dma((messages,))] * 2
        + [dma((messages, PIECES))] * 4
        + [dma((messages,))] * 2,
        compiler_params=pltpu.CompilerParams(
            collective_id=0, has_side_effects=True, vmem_limit_bytes=56 * 1024 * 1024
        ),
    )(
        step_gaps,
        window_start,
        table,
        freq,
        matrix,
        start_state.reshape(chunked),
        noise_draws.reshape(chunked),
        input_weight,
        embed_weight,
        first_weight,
        second_weight,
        output_weight,
    )
    return out.reshape((1,) + start_state.shape)


def solution(mesh):
    steps, inner = mesh.shape["steps"], mesh.shape["inner"]
    return jax.shard_map(
        functools.partial(shards, steps, inner),
        mesh=mesh,
        in_specs=(
            P("groups", None, None),
            P(("groups", "steps", "inner"), None, None, None),
            P(("groups", "steps", "inner")),
            P("groups"),
            P(),
            P(),
            P(),
            P(),
            P(),
        ),
        out_specs=P(("groups", "steps", "inner"), None, None, None),
        check_vma=False,
    )
```
